128 devices in a mesh: dp: 8 (over x, core), tensor: 16 (over y, z).
Axes of the slice: x: 4, y: 4, z: 4, core: 2. Of those that a mesh axis runs over, the one named last changes fastest.
Arguments:
- hidden: bfloat16 [16, 64, 4608], P('dp', 'tensor'), may hold values from -6 to 6
- gain: float32 [4608], replicated, may hold values from 0.5 to 1.5
- labels: int32 [16, 64], P('dp', 'tensor'), may hold values from 0 to 255999
- lengths: int32 [16], replicated, may hold values from 1 to 64
- embed: bfloat16 [256000, 4608], P(('dp', 'tensor')), may hold values from -0.375 to 0.375
Outputs:
- token_logprob: float32 [16, 64], P('dp', 'tensor')
- mean_nll: float32 [], replicated
- z_loss: float32 [], replicated
The draws below stay inside these ranges and needn't reach their ends.
All inputs are finite; a program needn't handle non-finite values.
Results may differ from the reference program's by a relative error of at most 0.00058.
Values may be sent and summed in bfloat16 or wider, within the bound.
No kernel may reach another device: no remote copies, remote signals or barrier semaphores. Data moves between devices by JAX's collectives and lax.ppermute only.
A program may use at most 128 MiB of HBM per device.

```python
import jax
import jax.numpy as jnp
from jax import lax

D = 4608
VOCAB = 256000
CAP = 30
LENGTH = 64
BATCH = 16


def set_ends(drawn, stream_key, least, largest):
    longest = drawn.shape.index(max(drawn.shape))
    spots = []
    for shift in (0, 1):
        where = [jax.random.randint(jax.random.fold_in(stream_key, axis), (), 0, length) for axis, length in enumerate(drawn.shape)]
        where[longest] = (where[longest] + shift) % drawn.shape[longest]
        spots.append(tuple(where))
    return drawn.at[spots[0]].set(least).at[spots[1]].set(largest)


def steps_of(key, dims, split, low, high):
    loudness = 1.0
    for axis_at, shards_of in split:
        steps = jax.random.uniform(jax.random.fold_in(jax.random.fold_in(key, 6), axis_at), (shards_of,), jnp.float32, low / len(split), high / len(split))
        loudness = loudness * jnp.repeat(jnp.exp(steps), dims[axis_at] // shards_of).reshape((-1,) + (1,) * (len(dims) - 1 - axis_at))
    return loudness


def normal_values(rng, dims, deviation, reach, pieces=(), dtype=jnp.bfloat16):
    drawn = jax.random.normal(rng, dims, jnp.float32) * deviation
    if len(pieces) > 0:
        drawn = steps_of(rng, dims, pieces, -0.22, 0.18) * drawn
    return jnp.clip(drawn, min=-reach, max=reach).astype(dtype)


def setup_inputs(seed: int = 0) -> dict:
    splits = jax.random.split(jax.random.key(seed), 6)
    hidden = normal_values(splits[0], (BATCH, LENGTH, D), 1.0, 6.0, ((0, 8), (1, 16)))
    gain = jnp.clip(1.0 + 0.1 * jax.random.normal(splits[1], (D,), jnp.float32), 0.5, 1.5)
    labels = set_ends(jax.random.randint(splits[2], (BATCH, LENGTH), 0, VOCAB), jax.random.fold_in(splits[2], 1), 0, VOCAB - 1).astype(jnp.int32)
    lengths = set_ends(jax.random.randint(splits[3], (BATCH,), 1, LENGTH + 1), jax.random.fold_in(splits[3], 1), 1, LENGTH).astype(jnp.int32)
    embed = normal_values(splits[4], (VOCAB, D), (D // 16) ** -0.5, 0.375, ((0, 128),))
    return dict(hidden=hidden, gain=gain, labels=labels, lengths=lengths, embed=embed)


def normalize(rows, gain):
    values = rows.astype(jnp.float32)
    meansq = lax.optimization_barrier(jnp.mean(values * values, axis=-1, keepdims=True))
    return (values * lax.rsqrt(meansq + 1e-06) * gain).astype(jnp.bfloat16)

def reference(hidden, gain, labels, lengths, embed):
    total_rows = BATCH * LENGTH
    normed = normalize(hidden.reshape(total_rows, D), gain)
    flat_labels = labels.reshape(total_rows)
    blocks = 32
    width = VOCAB // blocks
    table = embed.reshape(blocks, width, D)

    def visit(carry, item):
        sumexp, picked = carry
        tile, offset = item
        raw = lax.dot_general(normed, tile, (((1,), (1,)), ((), ())), preferred_element_type=jnp.float32)
        capped = CAP * jnp.tanh(raw / CAP)
        sumexp = sumexp + lax.optimization_barrier(jnp.sum(jnp.exp(capped), axis=1))
        local = flat_labels - offset
        inside = (local >= 0) & (local < width)
        chosen = jnp.take_along_axis(capped, jnp.clip(local, 0, width - 1)[:, None], axis=1)[:, 0]
        picked = picked + jnp.where(inside, chosen, jnp.float32(0.0))
        return ((sumexp, picked), None)
    offsets = (jnp.arange(blocks) * width).astype(jnp.int32)
    start = (jnp.zeros((total_rows,), jnp.float32), jnp.zeros((total_rows,), jnp.float32))
    (sumexp, picked), _ = lax.scan(visit, start, (table, offsets))
    lse = jnp.log(sumexp)
    positions = jnp.arange(LENGTH).astype(jnp.int32)
    live = (positions[None, :] < lengths[:, None]).astype(jnp.float32).reshape(total_rows)
    token = live * (picked - lse)
    count = jnp.sum(live)
    mean_nll = -jnp.sum(token) / count
    z_loss = 0.01 * jnp.sum(live * lse * lse) / count
    return (token.reshape(BATCH, LENGTH), mean_nll, z_loss)
```

```python
import jax
import jax.numpy as jnp
from jax import lax
from jax.experimental import pallas as pl
from jax.experimental.pallas import tpu as pltpu
from jax.sharding import Mesh
from jax.sharding import PartitionSpec as P

CAP = 30.0
TENSOR = ("tensor_0", "tensor_1")
DP = ("dp_0", "dp_1")
ALL = ("dp_0", "dp_1", "tensor_0", "tensor_1")
NX, NC, NY, NZ = 4, 2, 4, 4
LANES = 128
VOCAB_BLOCK = 400
MIB = 2**20


VMEM = pl.BlockSpec(memory_space=pltpu.VMEM)
SMEM = pl.BlockSpec(memory_space=pltpu.SMEM)


def pairs(kind, step):
    out = []
    for x in range(NX):
        for c in range(NC):
            for y in range(NY):
                for z in range(NZ):
                    tx, tc, ty, tz = x, c, y, z
                    if kind == "z":
                        tz = (z + step) % NZ
                    elif kind == "c":
                        tc = 1 - c
                    elif (kind == "u") == (c == 0):
                        tx = (x + step) % NX
                    else:
                        ty = (y + step) % NY
                    out.append((((x * NC + c) * NY + y) * NZ + z, ((tx * NC + tc) * NY + ty) * NZ + tz))
    return out


def move(value, kind, step=1):
    return lax.ppermute(value, ALL, pairs(kind, step))


def from_ring(value, kind):
    one = move(value, kind, 1)
    three = move(value, kind, -1)
    two = move(value, kind, 2)
    return one, two, three


def params(mib):
    return pltpu.CompilerParams(vmem_limit_bytes=mib * MIB)


def norm_body(labels, hidden, gain, out):
    width = hidden.shape[2]
    seqs, stretch = hidden.shape[0], hidden.shape[1]
    rows = seqs * stretch
    for s in range(seqs):
        values = hidden[s].astype(jnp.float32)
        meansq = jnp.mean(values * values, axis=-1, keepdims=True)
        normed = values * lax.rsqrt(meansq + 1e-06) * gain[...]
        out[s * stretch : (s + 1) * stretch, :width] = normed.astype(jnp.bfloat16)
    row = lax.broadcasted_iota(jnp.int32, (rows, LANES), 0)
    lane = lax.broadcasted_iota(jnp.int32, (rows, LANES), 1)
    label = jnp.zeros((rows, LANES), jnp.int32)
    for r in range(rows):
        label = jnp.where(row == r, labels[r // stretch, r % stretch], label)
    digit = jnp.where(lane == 0, label >> 16, jnp.where(lane == 1, (label >> 8) & 255, label & 255))
    digit = jnp.where(lane < 3, digit, 0)
    out[:, width:] = digit.astype(jnp.float32).astype(jnp.bfloat16)


def norm_call(labels, hidden, gain):
    seqs, stretch, width = hidden.shape
    return pl.pallas_call(
        norm_body,
        out_shape=jax.ShapeDtypeStruct((seqs * stretch, width + LANES), jnp.bfloat16),
        in_specs=[SMEM, VMEM, VMEM],
        out_specs=VMEM,
        compiler_params=params(4),
        name="norm",
    )(labels, hidden, gain)


def head_rows(first, embed, a, b, rows_ref):
    width = embed.shape[1]
    vocab = embed.shape[0]
    half = a.shape[0]
    rows_ref[0:half, :] = a[:, :width]
    rows_ref[half:, :] = b[:, :width]
    lane = lax.broadcasted_iota(jnp.int32, (8, LANES), 1)
    weight = jnp.where(lane == 0, 65536.0, jnp.where(lane == 1, 256.0, jnp.where(lane == 2, 1.0, 0.0)))
    weight = weight.astype(jnp.bfloat16)
    spread = (((1,), (1,)), ((), ()))
    label = jnp.concatenate(
        [
            lax.dot_general(weight, t[:, width:], spread, preferred_element_type=jnp.float32)[0:1]
            for t in (a, b)
        ],
        axis=1,
    )
    local = label.astype(jnp.int32) - first[0]
    sumexp = jnp.zeros((1, 2 * half), jnp.float32)
    picked = jnp.zeros((1, 2 * half), jnp.float32)
    for k in range(0, vocab, VOCAB_BLOCK):
        raw = lax.dot_general(
            embed[k : k + VOCAB_BLOCK, :], rows_ref[...], spread, preferred_element_type=jnp.float32
        )
        capped = CAP * jnp.tanh(raw * (1.0 / CAP))
        entry = lax.broadcasted_iota(jnp.int32, raw.shape, 0) + k
        sumexp += jnp.sum(jnp.exp(capped), axis=0, keepdims=True)
        picked += jnp.sum(jnp.where(entry == local, capped, 0.0), axis=0, keepdims=True)
    return sumexp, picked


def head_body(first, embed, a, b, out, rows_ref):
    sumexp, picked = head_rows(first, embed, a, b, rows_ref)
    out[0:1, :] = sumexp
    out[1:2, :] = picked


def last_body(first, embed, a, b, k1, k2, k3, out, rows_ref):
    last = head_rows(first, embed, a, b, rows_ref)
    half = a.shape[0]
    for stat in range(2):
        base = stat * 8
        s = slice(stat, stat + 1)
        out[base + 0 : base + 1, :] = k1[s, :half]
        out[base + 1 : base + 2, :] = k2[s, :half]
        out[base + 2 : base + 3, :] = last[stat][:, :half]
        out[base + 3 : base + 4, :] = k2[s, half:]
        out[base + 4 : base + 5, :] = k1[s, half:]
        out[base + 5 : base + 6, :] = k3[s, :half]
        out[base + 6 : base + 7, :] = last[stat][:, half:]
        out[base + 7 : base + 8, :] = k3[s, half:]


def head_call(first, embed, a, b, before=()):
    half = a.shape[0]
    vocab, width = embed.shape
    shape = (16, half) if before else (2, 2 * half)
    return pl.pallas_call(
        last_body if before else head_body,
        out_shape=jax.ShapeDtypeStruct(shape, jnp.float32),
        in_specs=[SMEM] + [VMEM] * (3 + len(before)),
        out_specs=VMEM,
        scratch_shapes=[pltpu.VMEM((2 * half, width), jnp.bfloat16)],
        compiler_params=params(12),
        cost_estimate=pl.CostEstimate(
            flops=4 * half * vocab * width,
            transcendentals=4 * half * vocab,
            bytes_accessed=2 * vocab * width,
        ),
        name="head_last" if before else "head",
    )(first, embed, a, b, *before)


def roll_lanes(t, k):
    return pltpu.roll(t, k % LANES, 1)


def roll_z(t, k):
    lane = lax.broadcasted_iota(jnp.int32, t.shape, 1) % 32
    return jnp.where(lane >= 8 * k, roll_lanes(t, 8 * k), roll_lanes(t, 8 * k - 32))


def roll_rows(t, k):
    return jnp.concatenate([t[4 - k :], t[: 4 - k]], axis=0)


def by_half(t, k, own_lanes):
    parts = []
    for g in range(4):
        part = t[4 * g : 4 * g + 4]
        parts.append(roll_lanes(part, 32 * k) if (g % 2 == 0) == own_lanes else roll_rows(part, k))
    return jnp.concatenate(parts, axis=0)


def place(t, kind, k):
    if kind == "z":
        return roll_z(t, k)
    return by_half(t, k, kind == "u")


def ring_sum(own, one, two, three, kind):
    return (own + place(two, kind, 2)) + (place(one, kind, 1) + place(three, kind, 3))


def core_body(own, other, out):
    t = other[...]
    out[...] = own[...] + jnp.concatenate([t[4:8], t[0:4], t[12:16], t[8:12]], axis=0)


def ring_body(kind):
    def body(own, one, two, three, out):
        out[...] = ring_sum(own[...], one[...], two[...], three[...], kind)

    return body


def small_call(body, name, *args):
    return pl.pallas_call(
        body,
        out_shape=jax.ShapeDtypeStruct(args[0].shape, args[0].dtype),
        in_specs=[VMEM] * len(args),
        out_specs=VMEM,
        compiler_params=params(2),
        name=name,
    )(*args)


def even_sum(t):
    t = t + roll_z(t, 2)
    t = t + roll_z(t, 1)
    t = t + roll_lanes(t, 64)
    t = t + roll_lanes(t, 32)
    halves = []
    for g in range(2):
        r = [t[4 * g + i : 4 * g + i + 1] for i in range(4)]
        halves.append((r[0] + r[2]) + (r[1] + r[3]))
    t = halves[0] + halves[1]
    for k in (4, 2, 1):
        t = t + roll_lanes(t, k)
    return t[:, 0:1]


def final_body(at, lengths, own, one, two, three, token_out, nll_out, z_out):
    total = ring_sum(own[...], one[...], two[...], three[...], "v")
    x, c, y, z = at[0], at[1], at[2], at[3]
    shape = (8, LANES)
    row = lax.broadcasted_iota(jnp.int32, shape, 0)
    lane = lax.broadcasted_iota(jnp.int32, shape, 1)
    other = row // 4
    v = row % 4
    u = lane // 32
    core = jnp.where(other == 1, 1 - c, c)
    at_x = (x + 4 - jnp.where(core == 0, u, v)) % 4
    at_y = (y + 4 - jnp.where(core == 0, v, u)) % 4
    at_z = (z + 4 - (lane // 8) % 4) % 4
    r = lane % 8
    seq = (at_x * 2 + core) * 2 + r // 4
    position = (at_y * 4 + at_z) * 4 + r % 4
    length = jnp.zeros(shape, jnp.int32)
    for s in range(lengths.shape[0]):
        length = jnp.where(seq == s, lengths[s], length)
    live = jnp.where(position < length, 1.0, 0.0).astype(jnp.float32)
    lse = jnp.log(total[0:8])
    token = live * (total[8:16] - lse)
    token_out[0:1, :] = token[0:1, 0:4]
    token_out[1:2, :] = token[0:1, 4:8]
    count = even_sum(live)
    nll_out[...] = -even_sum(token) / count
    z_out[...] = 0.01 * even_sum(live * lse * lse) / count


def final_call(at, lengths, own, one, two, three):
    scalar = jax.ShapeDtypeStruct((1, 1), jnp.float32)
    return pl.pallas_call(
        final_body,
        out_shape=(jax.ShapeDtypeStruct((2, 4), jnp.float32), scalar, scalar),
        in_specs=[SMEM, SMEM] + [VMEM] * 4,
        out_specs=(VMEM, VMEM, VMEM),
        compiler_params=params(2),
        name="final",
    )(at, lengths, own, one, two, three)


def per_device(hidden, gain, labels, lengths, embed):
    at = jnp.stack([lax.axis_index(a) for a in ALL]).astype(jnp.int32)
    first = (lax.axis_index(ALL) * embed.shape[0]).astype(jnp.int32)[None]
    own = norm_call(labels, hidden, gain[None])
    line = jnp.concatenate([own, *from_ring(own, "z")], axis=0)
    plane = jnp.concatenate([line, *from_ring(line, "u")], axis=0)
    one, two, three = from_ring(plane, "v")
    plane_c, one_c, three_c, two_c = (move(t, "c") for t in (plane, one, three, two))
    k1 = head_call(first, embed, plane, plane_c)
    k2 = head_call(first, embed, one, three)
    k3 = head_call(first, embed, one_c, three_c)
    stats = head_call(first, embed, two, two_c, (k1, k2, k3))
    stats = small_call(core_body, "core_sum", stats, move(stats, "c"))
    stats = small_call(ring_body("z"), "z_sum", stats, *from_ring(stats, "z"))
    stats = small_call(ring_body("u"), "u_sum", stats, *from_ring(stats, "u"))
    token, mean_nll, z_loss = final_call(at, lengths, stats, *from_ring(stats, "v"))
    return token, mean_nll[0, 0], z_loss[0, 0]


def solution(mesh):
    finer = Mesh(mesh.devices.reshape(NX, NC, NY, NZ), ALL)
    return jax.shard_map(
        per_device,
        mesh=finer,
        in_specs=(P(DP, TENSOR, None), P(), P(DP, TENSOR), P(), P(ALL, None)),
        out_specs=(P(DP, TENSOR), P(), P()),
        check_vma=False,
    )
```
